32 devices in a mesh: freq: 8 (over y, x, core), base: 4 (over z).
Axes of the slice: x: 2, y: 2, z: 4, core: 2. Of those that a mesh axis runs over, the one named last changes fastest.
Arguments:
- visibility: float32 [2, 16, 2048], P(None, 'freq', 'base'), may hold values from -6 to 6
- tile_of: int32 [16, 2048, 1], P('freq', 'base'), may hold values from 0 to 3; in each aligned block of 512 rows (0 to 511, 512 to 1023, ..., all dimensions but the last counted through in order) at most 256 rows name the same one
- u_within: int32 [16, 2048], P('freq', 'base'), may hold values from 0 to 255
- v_cell: int32 [16, 2048], P('freq', 'base'), may hold values from 0 to 1016
- kernel_index: int32 [2, 16, 2048], P(None, 'freq', 'base'), may hold values from 0 to 127
- kernel: float32 [128, 8], replicated, may hold values from 0.1 to 1
- live_count: int32 [16, 4], P('freq', 'base'), may hold values from 64 to 512, as said below
- bin_map: int32 [1024, 1024], P('base'), may hold values from 0 to 511, as said below
Outputs:
- power_map: float32 [1024, 1024], P('freq', 'base')
- spectrum: float32 [512], replicated
The draws below stay inside these ranges and needn't reach their ends.
Inputs may be any that keep to these rules, and one draw needn't show every extreme that they name: `tile_of`: among the visibilities of one channel on one device, at most 256 name the same tile, and in some device's visibilities a tile is named by exactly 256. `live_count`: the first device along base holds 512 used slots in every channel; the used slots of a device are its first ones. `bin_map`: every bin number occurs.
All inputs are finite; a program needn't handle non-finite values.
Results may differ from the reference program's by a relative error of at most 0.0003.
Values sent between devices are 32-bit elements; how exact they have to be, the bound alone decides.
A program may use at most 128 MiB of HBM per device.

```python
import math
import jax
import jax.numpy as jnp
import numpy as np
from jax import lax

G = 1024
NBINS = 512
KW = 8
OVER = 128
VIS_DEV = 512
CH_DEV = 2
TILE = 256
CAP = 256
CH = 16
VIS = 2048
N_FREQ = 8
N_BASE = 4


def draw_visibility(key, part):
    channels = CH_DEV * N_FREQ
    visits = VIS_DEV * N_BASE
    frequency = 100.0 + 60.0 * jnp.arange(channels, dtype=jnp.float32) / max(channels - 1, 1)
    falloff = (frequency / 100.0) ** (-2.6)
    values = jnp.clip(jax.random.normal(key, (2, channels, visits), jnp.float32), -6.0, 6.0)
    return values * falloff[None, :, None]


def draw_live_count(key, part):
    channels = CH_DEV * N_FREQ
    floor_count = VIS_DEV // 8
    device = jnp.arange(N_BASE, dtype=jnp.int32)
    spread = (VIS_DEV - floor_count) * (N_BASE - device) // N_BASE + 1
    additional = jax.random.randint(key, (channels, N_BASE), 0, spread[None, :])
    counts = floor_count + additional
    return jnp.where(device[None, :] == 0, VIS_DEV, counts).astype(jnp.int32)


def draw_bin_map(key, part):
    centre = jax.random.randint(key, (2,), -(G // 8), G // 8 + 1)
    positions = jnp.arange(G, dtype=jnp.int32)
    along_u = (positions - centre[0] + G // 2) % G - G // 2
    along_v = (positions - centre[1] + G // 2) % G - G // 2
    radius_sq = along_u[:, None] * along_u[:, None] + along_v[None, :] * along_v[None, :]
    return jnp.minimum(radius_sq * NBINS // (G // 2 * (G // 2)), NBINS - 1).astype(jnp.int32)


def plant(entries, stream_key, low, high):
    extent = entries.shape
    spot = [jax.random.randint(jax.random.fold_in(stream_key, axis), (), 0, extent[axis]) for axis in range(len(extent))]
    entries = entries.at[tuple(spot)].set(low)
    longest = extent.index(max(extent))
    spot[longest] = (spot[longest] + 1) % extent[longest]
    return entries.at[tuple(spot)].set(high)


def deal_out(key, own, number, rows, number_of, top, bound, slope):
    order = jax.random.permutation(key, number_of)
    heavy_load, usual = shares(number_of, rows * top, bound, slope, True), shares(number_of, rows * top, bound, slope, False)
    places = jnp.arange(number_of)

    def named(tallies, rotation):
        used = int((tallies > 0).sum())
        fixed = max(1, used // 4)
        passed = fixed + (places - fixed + rotation * (used - fixed)) % max(1, number_of - fixed)
        return jnp.zeros((number_of,), jnp.int32).at[order[jnp.where(places < fixed, places, passed)]].set(jnp.asarray(tallies, jnp.int32))

    tallies = jnp.where(number % 4 == 0, named(heavy_load, number // 4), named(usual, number - number // 4 - 1))
    mixed = jax.random.permutation(jax.random.fold_in(own, 3), number_of)
    giver, receiver = mixed[0:number_of // 2 * 2:2], mixed[1:number_of // 2 * 2:2]
    margin = jnp.minimum(tallies[giver] - 1, bound - tallies[receiver]) // 2
    margin = jnp.where((giver == order[0]) | (receiver == order[0]) | (tallies[receiver] == 0), 0, jnp.maximum(margin, 0))
    passed = jax.random.randint(jax.random.fold_in(own, 4), (number_of // 2,), 0, 1 << 20) % (margin + 1)
    tallies = tallies.at[giver].add(-passed).at[receiver].add(passed)
    items = jnp.searchsorted(jnp.cumsum(tallies), jnp.arange(rows * top), side="right").astype(jnp.int32)
    table = items.reshape(top, rows).T
    table = table[jax.random.permutation(jax.random.fold_in(own, 1), rows)]
    rotation = jax.random.randint(jax.random.fold_in(own, 2), (rows, 1), 0, top)
    return jnp.take_along_axis(table, (jnp.arange(top)[None, :] + rotation) % top, axis=1)


def shares(count, total, limit, skew, full):
    loads = [(1 << 20) // math.isqrt(rank ** skew) + 1 for rank in range(1, count + 1)]
    largest = limit if full else min(limit, max(-(-total // count), total * loads[0] // sum(loads)))
    least = 1 if total - largest >= count - 1 else 0
    given, surplus = [largest] + [least] * (count - 1), total - largest - least * (count - 1)
    while surplus > 0:
        free = [i for i in range(1, count) if given[i] < largest] or [i for i in range(1, count) if given[i] < limit]
        pool, remaining = sum([loads[i] for i in free]), surplus
        for i in free:
            more = min(limit - given[i], max(1, remaining * loads[i] // pool), surplus)
            given[i] = given[i] + more
            surplus = surplus - more
    return np.array(given)


def setup_inputs(seed: int = 0) -> dict:
    key_list = jax.random.split(jax.random.key(seed), 9)
    visibility = draw_visibility(jax.random.fold_in(key_list[8], 71), 0)
    tile_of_keys = jax.random.split(jax.random.fold_in(key_list[1], 1), CH * VIS // VIS_DEV)
    tile_of_turns = jax.random.permutation(jax.random.fold_in(key_list[1], 3), CH * VIS // VIS_DEV)
    tile_of = jax.vmap(lambda own, number: deal_out(jax.random.fold_in(key_list[1], 2), own, number, VIS_DEV, N_BASE, 1, CAP, 2))(tile_of_keys, tile_of_turns).reshape((CH, VIS, 1))
    u_within = plant(jax.random.randint(key_list[2], (CH, VIS), 0, TILE), jax.random.fold_in(key_list[2], 1), 0, TILE - 1).astype(jnp.int32)
    v_cell = plant(jax.random.randint(key_list[3], (CH, VIS), 0, G - KW + 1), jax.random.fold_in(key_list[3], 1), 0, G - KW).astype(jnp.int32)
    kernel_index = plant(jax.random.randint(key_list[4], (2, CH, VIS), 0, OVER), jax.random.fold_in(key_list[4], 1), 0, OVER - 1).astype(jnp.int32)
    kernel = jnp.clip(jnp.exp(jax.random.uniform(key_list[5], (OVER, KW), jnp.float32, math.log(0.1), math.log(1.0))), 0.1, 1.0)
    live_count = draw_live_count(jax.random.fold_in(key_list[8], 71), 0)
    bin_map = draw_bin_map(jax.random.fold_in(key_list[8], 71), 0)
    return {"visibility": visibility, "tile_of": tile_of, "u_within": u_within, "v_cell": v_cell, "kernel_index": kernel_index, "kernel": kernel, "live_count": live_count, "bin_map": bin_map}


def channel_power(visibility_re, visibility_im, tile_row, u_within, v_cell, index_u, index_v, used_slots, kernel):
    tile_rows = G // N_BASE
    u_cell = jnp.minimum(tile_row * tile_rows + u_within, G - KW)
    position = jnp.arange(VIS_DEV * N_BASE, dtype=jnp.int32)
    holder = position // VIS_DEV
    is_live = (position % VIS_DEV) < used_slots[holder]
    zeroed = jnp.zeros_like(visibility_re)
    real_part = jnp.where(is_live, visibility_re, zeroed)
    imag_part = jnp.where(is_live, visibility_im, zeroed)
    taps_u = kernel[index_u]
    taps_v = kernel[index_v]
    weight = taps_u[:, :, None] * taps_v[:, None, :]
    offsets = jnp.arange(KW, dtype=jnp.int32)
    row_cells = jnp.broadcast_to(u_cell[:, None, None] + offsets[None, :, None], weight.shape)
    col_cells = jnp.broadcast_to(v_cell[:, None, None] + offsets[None, None, :], weight.shape)
    grid_re = jnp.zeros((G, G), jnp.float32).at[row_cells, col_cells].add(weight * real_part[:, None, None])
    grid_im = jnp.zeros((G, G), jnp.float32).at[row_cells, col_cells].add(weight * imag_part[:, None, None])
    transformed = jnp.fft.fft2(grid_re + 1j * grid_im)
    return transformed.real * transformed.real + transformed.imag * transformed.imag


def reference(visibility, tile_of, u_within, v_cell, kernel_index, kernel, live_count, bin_map):
    def accumulate(running, channel_items):
        vis_re, vis_im, tile_row, within, column, index_u, index_v, used_slots = channel_items
        return running + channel_power(vis_re, vis_im, tile_row, within, column, index_u, index_v, used_slots, kernel), None

    channel_items = (visibility[0], visibility[1], tile_of[:, :, 0], u_within, v_cell, kernel_index[0], kernel_index[1], live_count)
    power_sum, _ = lax.scan(accumulate, jnp.zeros((G, G), jnp.float32), channel_items)
    channels = CH_DEV * N_FREQ
    visits = VIS_DEV * N_BASE
    power_map = power_sum / (channels * visits)
    flat_bins = bin_map.T.reshape(-1)
    totals = jax.ops.segment_sum(power_map.reshape(-1), flat_bins, num_segments=NBINS)
    counts = jax.ops.segment_sum(jnp.ones_like(power_map).reshape(-1), flat_bins, num_segments=NBINS)
    return power_map, totals / counts
```

```python
import functools
import math

import jax
import jax.numpy as jnp
import numpy as np
from jax import lax
from jax.experimental import pallas as pl
from jax.experimental.pallas import tpu as pltpu
from jax.sharding import PartitionSpec as P

NBINS = 512
BIN_LOW = 32
KW = 8
FINE = 32
SPREAD = FINE + KW
RADIX = 4
GROUP = 16


def halves_of(x):
    high = x.astype(jnp.bfloat16)
    low = (x - high.astype(jnp.float32)).astype(jnp.bfloat16)
    return high, low


def numpy_halves(x):
    x = np.asarray(x, np.float32)
    high = x.astype(jnp.bfloat16)
    low = (x - high.astype(np.float32)).astype(jnp.bfloat16)
    return high, low


def turn(product, grid):
    angle = (product % grid) * (2.0 * math.pi / grid)
    return np.cos(angle), np.sin(angle)


@functools.lru_cache(None)
def tables(grid, blocks):
    width = grid // blocks
    l = np.arange(grid)
    c, s = turn(np.arange(SPREAD)[:, None] * l[None, :], grid)
    c, s = (x.reshape(SPREAD, blocks, width) for x in (c, s))
    fine = np.concatenate(
        [np.concatenate([c, -s], axis=2), np.concatenate([s, c], axis=2)], axis=0
    ).transpose(1, 0, 2)
    fh, fl = numpy_halves(fine)
    pad = np.zeros((blocks, 256 - 6 * SPREAD, 2 * width), fh.dtype)
    fine = np.concatenate([fh, fl, fh, pad], axis=1)
    coarse_count = grid // FINE
    c, s = turn(np.arange(coarse_count)[:, None] * FINE * l[None, :], grid)
    c, s = (x.reshape(coarse_count, blocks, width) for x in (c, s))
    ch, cl = numpy_halves(np.concatenate([c, -s], axis=2).transpose(1, 0, 2))
    coarse = np.concatenate([ch, cl], axis=1)
    slab = grid // RADIX
    u = RADIX * np.arange(slab)[None, None, :] + np.arange(RADIX)[:, None, None]
    c, s = turn(np.arange(slab)[None, :, None] * u, grid)
    dh, dl = numpy_halves(np.concatenate([c, s], axis=1))
    return fine, coarse, dh, dl


def dot(a, b):
    return jnp.dot(a, b, preferred_element_type=jnp.float32)


def dot_slots(a, b):
    return lax.dot_general(a, b, (((0,), (0,)), ((), ())), preferred_element_type=jnp.float32)


def image_kernel(
    grid, scale, f_ref, fine_ref, coarse_ref, dh_ref, dl_ref, out_ref, q_ref, rh_ref, rl_ref,
    wh_ref, wl_ref, zh_ref, zl_ref, h_ref, y_ref
):
    channel, chunk = pl.program_id(0), pl.program_id(1)
    chunks = pl.num_programs(1)
    slots = f_ref.shape[2]
    width = out_ref.shape[1]
    slab = grid // RADIX
    period = RADIX * GROUP
    re, im = f_ref[0, 0:1, :], f_ref[0, 1:2, :]
    u = f_ref[0, 2:3, :].astype(jnp.int32)
    v = f_ref[0, 3:4, :].astype(jnp.int32)

    for first in range(RADIX):
        residue = RADIX * lax.broadcasted_iota(jnp.int32, (GROUP, slots), 0) + first
        tap = (residue - u) & (period - 1)
        group = (u + tap - residue) // period
        r = jnp.zeros((GROUP, slots), jnp.float32)
        for t in range(KW):
            r = jnp.where(tap == t, f_ref[0, 4 + t:5 + t, :], r)
        rh, rl = halves_of(r)
        q_ref[first] = group.astype(jnp.float32).astype(jnp.bfloat16)
        rh_ref[first] = rh
        rl_ref[first] = rl

    piece = min(512, slots)
    for start in range(0, slots, piece):
        at = slice(start, start + piece)
        vp = v[:, at]
        offset = lax.broadcasted_iota(jnp.int32, (SPREAD, piece), 0) - (vp & (FINE - 1))
        spread = jnp.zeros((SPREAD, piece), jnp.float32)
        for t in range(KW):
            spread = jnp.where(offset == t, f_ref[0, 4 + KW + t:5 + KW + t, at], spread)
        both = jnp.concatenate([spread * re[:, at], spread * im[:, at]], axis=0)
        bh, bl = halves_of(both)
        pad = jnp.zeros((256 - 6 * SPREAD, piece), jnp.bfloat16)
        zb = dot_slots(jnp.concatenate([bh, bh, bl, pad], axis=0), fine_ref[...])
        count = coarse_ref.shape[0]
        pick = lax.broadcasted_iota(jnp.int32, (count, piece), 0) & (count // 2 - 1)
        onehot = jnp.where(pick == vp // FINE, 1.0, 0.0).astype(jnp.bfloat16)
        e = dot_slots(onehot, coarse_ref[...])
        zr, zi = zb[:, :width], zb[:, width:]
        er, ei = e[:, :width], e[:, width:]
        z = jnp.concatenate([zr * er - zi * ei, zr * ei + zi * er], axis=1)
        zh, zl = halves_of(z)
        zh_ref[at, :] = zh
        zl_ref[at, :] = zl

    def slab_step(first, carry):
        q, rh, rl = q_ref[first], rh_ref[first], rl_ref[first]
        zero = jnp.zeros_like(rh)
        for g in range(slab // GROUP):
            hit = q == jnp.bfloat16(g)
            wh_ref[g * GROUP:(g + 1) * GROUP, :] = jnp.where(hit, rh, zero)
            wl_ref[g * GROUP:(g + 1) * GROUP, :] = jnp.where(hit, rl, zero)
        zh = zh_ref[...]
        wh = wh_ref[...]
        rows = dot(wh, zh) + dot(wh, zl_ref[...]) + dot(wl_ref[...], zh)

        @pl.when(chunk == 0)
        def _():
            h_ref[first] = rows

        @pl.when(chunk > 0)
        def _():
            h_ref[first] += rows

        return carry

    lax.fori_loop(0, RADIX, slab_step, 0)

    @pl.when((channel == 0) & (chunk == 0))
    def _():
        out_ref[...] = jnp.zeros_like(out_ref)

    @pl.when(chunk == chunks - 1)
    def _():
        def transform_step(first, carry):
            hh, hl = halves_of(h_ref[first])
            dh = dh_ref[first]
            y_ref[first] = dot(dh, hh) + dot(dh, hl) + dot(dl_ref[first], hh)
            return carry

        lax.fori_loop(0, RADIX, transform_step, 0)

        def combine(block, carry):
            rows = 32
            top = pl.multiple_of(block * rows, rows)
            low = pl.multiple_of(slab + block * rows, rows)
            yr, yi = [], []
            for first in range(RADIX):
                cy = y_ref[first, pl.ds(top, rows), :]
                sy = y_ref[first, pl.ds(low, rows), :]
                yr.append(cy[:, :width] + sy[:, width:])
                yi.append(cy[:, width:] - sy[:, :width])
            ar, ai = yr[0] + yr[2], yi[0] + yi[2]
            br, bi = yr[0] - yr[2], yi[0] - yi[2]
            cr, ci = yr[1] + yr[3], yi[1] + yi[3]
            dr, di = yr[1] - yr[3], yi[1] - yi[3]
            parts = [
                (ar + cr, ai + ci), (br + di, bi - dr), (ar - cr, ai - ci), (br - di, bi + dr)
            ]
            for k, (xr, xi) in enumerate(parts):
                at = pl.ds(pl.multiple_of(k * slab + block * rows, rows), rows)
                out_ref[at, :] += (xr * xr + xi * xi) * scale
            return carry

        lax.fori_loop(0, slab // 32, combine, 0)


def image_power(fields, fine, coarse, dh, dl, grid, scale):
    channels, field_count, total = fields.shape
    width = fine.shape[1] // 2
    chunk = min(2048, total)
    slab = grid // RADIX
    bf16, f32 = jnp.bfloat16, jnp.float32
    full = lambda x: pl.BlockSpec(x.shape, lambda c, n: (0,) * x.ndim)
    return pl.pallas_call(
        functools.partial(image_kernel, grid, scale),
        grid=(channels, total // chunk),
        out_shape=jax.ShapeDtypeStruct((grid, width), f32),
        in_specs=[
            pl.BlockSpec((1, field_count, chunk), lambda c, n: (c, 0, n)),
            full(fine), full(coarse), full(dh), full(dl),
        ],
        out_specs=pl.BlockSpec((grid, width), lambda c, n: (0, 0)),
        scratch_shapes=[
            pltpu.VMEM((RADIX, GROUP, chunk), bf16),
            pltpu.VMEM((RADIX, GROUP, chunk), bf16),
            pltpu.VMEM((RADIX, GROUP, chunk), bf16),
            pltpu.VMEM((slab, chunk), bf16),
            pltpu.VMEM((slab, chunk), bf16),
            pltpu.VMEM((chunk, 2 * width), bf16),
            pltpu.VMEM((chunk, 2 * width), bf16),
            pltpu.VMEM((RADIX, slab, 2 * width), f32),
            pltpu.VMEM((RADIX, 2 * slab, 2 * width), f32),
        ],
        compiler_params=pltpu.CompilerParams(
            vmem_limit_bytes=60 * 2**20, dimension_semantics=("arbitrary", "arbitrary")
        ),
    )(fields, fine, coarse, dh, dl)


def histogram_kernel(power_ref, bins_ref, out_ref, a_ref, b_ref):
    rows, columns = power_ref.shape
    high_count = NBINS // BIN_LOW
    bins = bins_ref[...].T
    for k in range(rows):
        at = slice(k * columns, (k + 1) * columns)
        value = power_ref[k:k + 1, :]
        bin_id = bins[k:k + 1, :]
        hit = lax.broadcasted_iota(jnp.int32, (high_count, columns), 0) == bin_id // BIN_LOW
        high = value.astype(jnp.bfloat16).astype(jnp.float32)
        low = value - high
        a_ref[0:high_count, at] = jnp.where(hit, high, 0.0).astype(jnp.bfloat16)
        a_ref[high_count:2 * high_count, at] = jnp.where(hit, low, 0.0).astype(jnp.bfloat16)
        a_ref[2 * high_count:, at] = jnp.where(hit, 1.0, 0.0).astype(jnp.bfloat16)
        hit = lax.broadcasted_iota(jnp.int32, (BIN_LOW, columns), 0) == bin_id % BIN_LOW
        b_ref[:, at] = jnp.where(hit, 1.0, 0.0).astype(jnp.bfloat16)
    sums = lax.dot_general(
        a_ref[...], b_ref[...], (((1,), (1,)), ((), ())), preferred_element_type=jnp.float32
    )
    out_ref[0] = sums[:high_count] + sums[high_count:2 * high_count]
    out_ref[1] = sums[2 * high_count:]


def histogram(power, bins):
    high_count = NBINS // BIN_LOW
    return pl.pallas_call(
        histogram_kernel,
        out_shape=jax.ShapeDtypeStruct((2, high_count, BIN_LOW), jnp.float32),
        scratch_shapes=[
            pltpu.VMEM((3 * high_count, power.size), jnp.bfloat16),
            pltpu.VMEM((BIN_LOW, power.size), jnp.bfloat16),
        ],
    )(power, bins)


def look_up_taps(kernel_index, kernel):
    rows = kernel.shape[0]
    onehot = (kernel_index[:, :, None, :] == jnp.arange(rows, dtype=jnp.int32)[:, None]).astype(
        jnp.float32
    )
    return jnp.einsum("acon,ot->actn", onehot, kernel, precision=lax.Precision.HIGHEST)


def per_device(visibility, tile_of, u_within, v_cell, kernel_index, kernel, live_count, bin_map):
    base_count = lax.axis_size("base")
    freq_count = lax.axis_size("freq")
    grid = bin_map.shape[1]
    tile_rows = grid // base_count
    channels_here, slots = u_within.shape
    fine, coarse, dh, dl = tables(grid, base_count)
    here = lax.axis_index("base")
    fine = lax.dynamic_index_in_dim(jnp.asarray(fine), here, 0, keepdims=False)
    coarse = lax.dynamic_index_in_dim(jnp.asarray(coarse), here, 0, keepdims=False)

    is_live = jnp.arange(slots, dtype=jnp.int32)[None, :] < live_count
    vis = jnp.where(is_live[None], visibility, 0.0)
    u_cell = jnp.minimum(tile_of[:, :, 0] * tile_rows + u_within, grid - KW)
    taps = look_up_taps(kernel_index, kernel)
    fields = jnp.concatenate(
        [
            vis.transpose(1, 0, 2),
            u_cell[:, None].astype(jnp.float32),
            v_cell[:, None].astype(jnp.float32),
            taps[0],
            taps[1],
            jnp.zeros((channels_here, 4, slots), jnp.float32),
        ],
        axis=1,
    )
    fields = lax.all_gather(fields, "base", axis=2, tiled=True)
    scale = 1.0 / (channels_here * freq_count * slots * base_count)
    power_part = image_power(fields, fine, coarse, jnp.asarray(dh), jnp.asarray(dl), grid, scale)
    share_rows = grid // freq_count
    power_share = lax.psum_scatter(power_part, "freq", scatter_dimension=0, tiled=True)
    bins_share = lax.dynamic_slice_in_dim(
        bin_map, lax.axis_index("freq") * share_rows, share_rows, 1
    )
    sums = lax.psum(histogram(power_share, bins_share), ("freq", "base"))
    return (power_share, (sums[0] / sums[1]).reshape(NBINS))


def solution(mesh):
    in_specs = (
        P(None, "freq", "base"),
        P("freq", "base", None),
        P("freq", "base"),
        P("freq", "base"),
        P(None, "freq", "base"),
        P(),
        P("freq", "base"),
        P("base", None),
    )
    out_specs = (P("freq", "base"), P())
    return jax.shard_map(
        per_device, mesh=mesh, in_specs=in_specs, out_specs=out_specs, check_vma=False
    )
```
